32 devices in a mesh: gx: 4 (over z), gy: 4 (over y, core), gz: 2 (over x).
Axes of the slice: x: 2, y: 2, z: 4, core: 2. Of those that a mesh axis runs over, the one named last changes fastest.
Arguments:
- coarse_source: float32 [64, 128, 256], P('gx', 'gy', 'gz'), may hold values from -6 to 6
- coarse_shift: float32 [64, 128, 256], P('gx', 'gy', 'gz'), may hold values from 0.1 to 4
- coarse_start: float32 [64, 128, 256], P('gx', 'gy', 'gz'), may hold values from -3 to 3
- fine_source: float32 [128, 32768], P(('gx', 'gy', 'gz')), may hold values from -6 to 6
- fine_shift: float32 [128, 32768], P(('gx', 'gy', 'gz')), may hold values from 0.1 to 4
- fine_start: float32 [128, 32768], P(('gx', 'gy', 'gz')), may hold values from -3 to 3
- box_corner: int32 [32, 4, 3], P(('gx', 'gy', 'gz')), may hold values from 0 to 480, as said below
- box_owner: int32 [32, 4], P(('gx', 'gy', 'gz')), may hold values from 0 to 8, as said below
Outputs:
- potential: float32 [64, 128, 256], P('gx', 'gy', 'gz')
- fine_solution: float32 [128, 32768], P(('gx', 'gy', 'gz'))
- residual_norms: float32 [2], replicated
The draws below stay inside these ranges and needn't reach their ends.
Inputs may be any that keep to these rules, and one draw needn't show every extreme that they name: `box_owner`: each device has at least one live slot; in every group of 8 devices that share a gx index some device has 4 live slots; the live owners of one device are distinct; no device is the owner of more than 4 live boxes, and in every group some device is the owner of exactly 4 live boxes. `box_corner`: each corner is a multiple of 32 and its footprint lies in the coarse block of the device that lists it; the 4 footprints of one device are distinct.
All inputs are finite; a program needn't handle non-finite values.
Results may differ from the reference program's by a relative error of at most 0.0001.
Values sent between devices are 32-bit elements; how exact they have to be, the bound alone decides.
A program may use at most 128 MiB of HBM per device.

```python
import math
import jax
import jax.numpy as jnp
from jax import lax

CX = 16
CY = 32
CZ = 128
FOOT = 16
SLOTS = 4
CYCLES = 2
CSWEEPS = 4
FSWEEPS = 3
FINE = 32768
BOXES = 128
NX = 64
NY = 128
NZ = 256
N_GY = 4
N_GZ = 2
DEVICES = 32


def draw_box_owner(key, part):
    group = N_GY * N_GZ
    keys = jax.random.split(jax.random.fold_in(key, 41), DEVICES // group)

    def choose(single):
        return jax.random.permutation(single, group)[:SLOTS].astype(jnp.int32)
    offsets = jnp.repeat(jax.vmap(choose)(keys), group, axis=0)
    heavy = jnp.repeat(jax.random.randint(jax.random.fold_in(key, 42), (DEVICES // group,), 0, group).astype(jnp.int32), group)
    counts = jax.random.randint(jax.random.fold_in(key, 11), (DEVICES,), 1, SLOTS + 1).astype(jnp.int32)
    rank = jnp.arange(DEVICES, dtype=jnp.int32) % group
    senders = (heavy[:, None] - offsets) % group
    full = jnp.any(senders == rank[:, None], axis=1)
    counts = jnp.where(full, SLOTS, counts).astype(jnp.int32)
    owners = ((rank[:, None] + offsets) % group).astype(jnp.int32)
    slot = jnp.arange(SLOTS, dtype=jnp.int32)[None, :]
    return jnp.where(slot < counts[:, None], owners, group).astype(jnp.int32)


def draw_box_corner(key, part):
    group = N_GY * N_GZ
    along_x = CX // FOOT
    along_y = CY // FOOT
    along_z = CZ // FOOT
    places = along_x * along_y * along_z
    keys = jax.random.split(jax.random.fold_in(key, 31), DEVICES)

    def choose(single):
        return jax.random.permutation(single, places)[:SLOTS].astype(jnp.int32)
    picked = jax.vmap(choose)(keys)
    device = jnp.arange(DEVICES, dtype=jnp.int32)[:, None]
    device_x = device // group
    device_y = device // N_GZ % N_GY
    device_z = device % N_GZ
    block_x = picked // (along_y * along_z)
    block_y = picked // along_z % along_y
    block_z = picked % along_z
    fine_x = 2 * (device_x * CX + block_x * FOOT)
    fine_y = 2 * (device_y * CY + block_y * FOOT)
    fine_z = 2 * (device_z * CZ + block_z * FOOT)
    return jnp.stack([fine_x, fine_y, fine_z], axis=-1).astype(jnp.int32)


def block_levels(stream_key, dims, shards, low, largest):
    loudness = 1.0
    for axis_at, blocks in shards:
        steps = jax.random.uniform(jax.random.fold_in(jax.random.fold_in(stream_key, 6), axis_at), (blocks,), jnp.float32, low / len(shards), largest / len(shards))
        loudness = loudness * jnp.repeat(jnp.exp(steps), dims[axis_at] // blocks).reshape((-1,) + (1,) * (len(dims) - 1 - axis_at))
    return loudness


def noise(rng, dims, deviation, limit, cuts=(), kind=jnp.bfloat16):
    result = jax.random.normal(rng, dims, jnp.float32) * deviation
    if len(cuts) > 0:
        result = block_levels(rng, dims, cuts, -0.22, 0.18) * result
    return jnp.clip(result, min=-limit, max=limit).astype(kind)


def setup_inputs(seed: int = 0) -> dict:
    seeds = jax.random.split(jax.random.key(seed), 9)
    coarse_source = noise(seeds[0], (NX, NY, NZ), 1.0, 6.0, ((0, 4), (1, 4), (2, 2)), jnp.float32)
    coarse_shift = jnp.clip(jnp.exp(math.log(4.0) - 3.6888794 * jax.random.uniform(seeds[1], (NX, NY, NZ), jnp.float32) ** block_levels(seeds[1], (NX, NY, NZ), ((0, 4), (1, 4), (2, 2)), -0.2, 0.2)), 0.1, 4.0)
    coarse_start = noise(seeds[2], (NX, NY, NZ), 0.5, 3.0, ((0, 4), (1, 4), (2, 2)), jnp.float32)
    fine_source = noise(seeds[3], (BOXES, FINE), 1.0, 6.0, ((0, 32),), jnp.float32)
    fine_shift = jnp.clip(jnp.exp(math.log(4.0) - 3.6888794 * jax.random.uniform(seeds[4], (BOXES, FINE), jnp.float32) ** block_levels(seeds[4], (BOXES, FINE), ((0, 32),), -0.2, 0.2)), 0.1, 4.0)
    fine_start = noise(seeds[5], (BOXES, FINE), 0.5, 3.0, ((0, 32),), jnp.float32)
    box_corner = draw_box_corner(jax.random.fold_in(seeds[8], 71), 0)
    box_owner = draw_box_owner(jax.random.fold_in(seeds[8], 71), 0)
    return {"coarse_source": coarse_source, "coarse_shift": coarse_shift, "coarse_start": coarse_start, "fine_source": fine_source, "fine_shift": fine_shift, "fine_start": fine_start, "box_corner": box_corner, "box_owner": box_owner}


OMEGA = 0.8

def to_blocks(field):
    extent = field.shape
    shaped = field.reshape(extent[0] // FOOT, FOOT, extent[1] // FOOT, FOOT, extent[2] // FOOT, FOOT)
    return shaped.transpose(0, 2, 4, 1, 3, 5).reshape(-1, FOOT * FOOT * FOOT)

def from_blocks(blocks, extent):
    shaped = blocks.reshape(extent[0] // FOOT, extent[1] // FOOT, extent[2] // FOOT, FOOT, FOOT, FOOT)
    return shaped.transpose(0, 3, 1, 4, 2, 5).reshape(extent)

def inject(parents):
    number = parents.shape[0]
    shaped = parents.reshape(number, FOOT, 1, FOOT, 1, FOOT, 1)
    spread = jnp.broadcast_to(shaped, (number, FOOT, 2, FOOT, 2, FOOT, 2))
    return spread.reshape(number, 8 * FOOT * FOOT * FOOT)

def restrict(values):
    number = values.shape[0]
    return values.reshape(number, FOOT, 2, FOOT, 2, FOOT, 2).mean(axis=(2, 4, 6)).reshape(number, FOOT * FOOT * FOOT)

def fine_residual(values, parents, source, shift):
    ghost = inject(parents)
    side = 2 * FOOT
    position = jnp.arange(side * side * side, dtype=jnp.int32)[None, :]
    summed = jnp.zeros_like(values)
    for stride in (1, side, side * side):
        coordinate = position // stride % side
        upper = jnp.roll(values, -stride, axis=1)
        lower = jnp.roll(values, stride, axis=1)
        summed = summed + jnp.where(coordinate < side - 1, upper, ghost) + jnp.where(coordinate > 0, lower, ghost)
    return source - (6.0 + shift) * values + summed

def beside_sum(padded):
    summed = padded[2:, 1:-1, 1:-1] + padded[:-2, 1:-1, 1:-1]
    summed = summed + padded[1:-1, 2:, 1:-1] + padded[1:-1, :-2, 1:-1]
    return summed + padded[1:-1, 1:-1, 2:] + padded[1:-1, 1:-1, :-2]

def reference(coarse_source, coarse_shift, coarse_start, fine_source, fine_shift, fine_start, box_corner, box_owner):
    group = N_GY * N_GZ
    device_ids = jnp.arange(DEVICES, dtype=jnp.int32)
    live = box_owner < group
    owner_safe = jnp.minimum(box_owner, group - 1).astype(jnp.int32)
    hit = ((box_owner[:, :, None] == jnp.arange(group, dtype=jnp.int32)[None, None, :]) & live[:, :, None]).astype(jnp.int32)
    incoming = lax.optimization_barrier(jnp.sum(hit, axis=1)).astype(jnp.int32)
    grouped = incoming.reshape(DEVICES // group, group, group)
    before = (jnp.cumsum(grouped, axis=1).astype(jnp.int32) - grouped).reshape(DEVICES, group).astype(jnp.int32)
    slot_j = jnp.take_along_axis(before, owner_safe, axis=1).astype(jnp.int32)
    owner_global = ((device_ids // group)[:, None] * group + owner_safe).astype(jnp.int32)
    rows = (owner_global * SLOTS + slot_j).astype(jnp.int32)
    targets = jnp.where(live, rows, BOXES).reshape(-1).astype(jnp.int32)
    block = (box_corner // 2 // FOOT).reshape(-1, 3)
    block_index = ((block[:, 0] * (NY // FOOT) + block[:, 1]) * (NZ // FOOT) + block[:, 2]).astype(jnp.int32)
    home_of_row = jnp.zeros((BOXES,), jnp.int32).at[targets].set(jnp.arange(DEVICES * SLOTS, dtype=jnp.int32), mode='drop')
    occupied = jnp.zeros((BOXES,), jnp.float32).at[targets].set(1.0, mode='drop')[:, None]
    row_block = block_index[home_of_row].astype(jnp.int32)
    source = fine_source
    shift = fine_shift
    values = fine_start
    fine_diagonal = 6.0 + shift
    diagonal = 6.0 + coarse_shift
    potential = coarse_start
    earlier = None
    norms = []
    for cycle in range(CYCLES):
        parents = to_blocks(potential)[row_block]
        if cycle > 0:
            values = values + inject(parents - earlier)
        for sweep in range(FSWEEPS):
            values = values + OMEGA * fine_residual(values, parents, source, shift) / fine_diagonal
        remainder = fine_residual(values, parents, source, shift)
        restricted = restrict(remainder) * occupied
        placed = jnp.zeros((NX // FOOT * (NY // FOOT) * (NZ // FOOT), FOOT * FOOT * FOOT), jnp.float32)
        placed = placed.at[row_block].add(restricted)
        composite = coarse_source + from_blocks(placed, coarse_source.shape)
        for sweep in range(CSWEEPS):
            residual = composite - diagonal * potential + beside_sum(jnp.pad(potential, 1))
            potential = potential + OMEGA * residual / diagonal
        squares = jnp.sum(residual * residual) + jnp.sum(occupied * remainder * remainder)
        norms.append(jnp.sqrt(squares / (NX * NY * NZ)))
        earlier = parents
    parents = to_blocks(potential)[row_block]
    fine_solution = (values + inject(parents - earlier)) * occupied
    return (potential, fine_solution, jnp.stack(norms))
```

```python
import functools

import jax
import jax.numpy as jnp
from jax import lax
from jax.experimental import pallas as pl
from jax.experimental.pallas import tpu as pltpu
from jax.sharding import PartitionSpec as P

FOOT = 16
CYCLES = 2
CSWEEPS = 4
FSWEEPS = 3
OMEGA = 0.8
KEEP = 1.0 - OMEGA
MESH = pl.DeviceIdType.MESH
LANES = 128
SIDE = 2 * FOOT


def take(x, idx):
    return jnp.take_along_axis(x, idx, axis=1, mode="promise_in_bounds")


def iota(shape, dim):
    return lax.broadcasted_iota(jnp.int32, shape, dim)


def kernel(
    sizes,
    corner,
    owner,
    c_src,
    c_shift,
    c_start,
    f_src,
    f_shift,
    f_start,
    pot_out,
    fine_out,
    norm_out,
    U,
    W,
    comp,
    yh,
    ys,
    zh,
    zs,
    V,
    FW,
    FS,
    G,
    compact,
    R,
    pout,
    prec,
    rout,
    rrec,
    slotid,
    sums,
    xsum,
    p_send,
    p_recv,
    r_send,
    r_recv,
    h_send,
    h_recv,
    n_send,
    n_recv,
):
    n_gx, n_gy, n_gz = sizes
    group = n_gy * n_gz
    slots = owner.shape[1]
    nx, ny, nz = c_src.shape
    along_y = ny // FOOT
    gx, gy, gz = lax.axis_index("gx"), lax.axis_index("gy"), lax.axis_index("gz")
    me = gy * n_gz + gz

    def rank_id(rank):
        return (gx, rank // n_gz, rank % n_gz)

    have = (gx > 0, gx < n_gx - 1, gy > 0, gy < n_gy - 1, gz > 0, gz < n_gz - 1)
    beside = (
        (gx - 1, gy, gz),
        (gx + 1, gy, gz),
        (gx, gy - 1, gz),
        (gx, gy + 1, gz),
        (gx, gy, gz - 1),
        (gx, gy, gz + 1),
    )

    for p in range(2):
        U[p, 0] = jnp.zeros((ny, nz), jnp.float32)
        U[p, nx + 1] = jnp.zeros((ny, nz), jnp.float32)
    yh[...] = jnp.zeros_like(yh)
    zh[...] = jnp.zeros_like(zh)

    barrier = pltpu.get_barrier_semaphore()
    for d in range(1, group):
        pl.semaphore_signal(barrier, inc=1, device_id=rank_id((me + d) % group), device_id_type=MESH)
    for d in range(1, n_gx):
        pl.semaphore_signal(barrier, inc=1, device_id=((gx + d) % n_gx, gy, gz), device_id_type=MESH)
    pl.semaphore_wait(barrier, group - 1 + n_gx - 1)

    tile = (8, LANES)
    lane = iota(tile, 1)
    sub = iota(tile, 0)
    wide = (ny, LANES)
    wlane = iota(wide, 1)
    wsub = iota(wide, 0)
    box_row = []
    box_col = []
    box_live = []
    for s in range(slots):
        box_row.append((corner[0, s, 1] // 2 - gy * ny) // FOOT)
        box_col.append((corner[0, s, 2] // 2 - gz * nz) // FOOT)
        box_live.append(owner[0, s] < group)

    def exchange(out, rec, send, recv, rows):
        copies = []
        for d in range(1, group):
            peer = (me + d) % group
            copy = pltpu.make_async_remote_copy(
                src_ref=out.at[peer, pl.ds(0, rows)],
                dst_ref=rec.at[me, pl.ds(0, rows)],
                send_sem=send.at[d],
                recv_sem=recv.at[d],
                device_id=rank_id(peer),
                device_id_type=MESH,
            )
            copy.start()
            copies.append(copy)
        rec[me, pl.ds(0, rows)] = out[me, pl.ds(0, rows)]
        return copies

    def arrive(out, rec, send, recv, rows):
        for d in range(1, group):
            source = (me + group - d) % group
            pltpu.make_async_remote_copy(
                src_ref=out.at[source, pl.ds(0, rows)],
                dst_ref=rec.at[source, pl.ds(0, rows)],
                send_sem=send.at[d],
                recv_sem=recv.at[d],
                device_id=rank_id(source),
                device_id_type=MESH,
            ).wait_recv()

    def pack_parents(p):
        @pl.loop(0, FOOT // 4)
        def _(xg):
            for s in range(slots):
                idx = box_col[s] * FOOT + (lane % FOOT)
                acc = jnp.zeros(tile, jnp.float32)
                for k in range(4):
                    for yl in range(2):
                        a = U[p, 1 + xg * 4 + k, pl.ds(yl, 8, stride=2), :]
                        for b in range(1, along_y):
                            other = U[p, 1 + xg * 4 + k, pl.ds(b * FOOT + yl, 8, stride=2), :]
                            a = jnp.where(box_row[s] == b, other, a)
                        acc = jnp.where(lane // FOOT == 2 * k + yl, take(a, idx), acc)
                compact[s, pl.ds(pl.multiple_of(xg * 8, 8), 8), :] = acc

        for q in range(group):
            acc = jnp.zeros((32, LANES), jnp.float32)
            flag = jnp.zeros(tile, jnp.float32)
            for s in range(slots):
                acc = jnp.where(owner[0, s] == q, compact[s], acc)
                flag = jnp.where(owner[0, s] == q, 1.0, flag)
            pout[q, pl.ds(0, 32)] = acc
            pout[q, pl.ds(32, 8)] = flag

    def slot_masks():
        count = jnp.zeros(tile, jnp.float32)
        for q in range(group):
            flag = prec[q, pl.ds(32, 8)]
            slotid[q] = jnp.where(flag > 0.5, count, -1.0)
            count = count + flag
        return count

    spread_lane = (lane // 64) * FOOT + (lane % SIDE) // 2

    def ghosts(par):
        @pl.loop(0, FOOT // 4)
        def _(xg):
            rows = pl.ds(pl.multiple_of(xg * 8, 8), 8)
            for j in range(slots):
                acc = jnp.zeros(tile, jnp.float32)
                for q in range(group):
                    acc = jnp.where(slotid[q] == float(j), prec[q, rows], acc)
                for k in range(4):
                    G[par, j, xg * 4 + k] = take(acc, k * SIDE + spread_lane)

    y_top = (lane >= 96) & (sub == 7)
    y_low = (lane < 32) & (sub == 0)
    z_pos = lane % SIDE

    def beside_fine(vp, par, j, x, ghost):
        v = V[vp, j, x + 1]
        up = pltpu.roll(v, LANES - 32, 1)
        up = jnp.where(lane < 96, up, pltpu.roll(up, 7, 0))
        up = jnp.where(y_top, ghost, up)
        lo = pltpu.roll(v, 32, 1)
        lo = jnp.where(lane >= 32, lo, pltpu.roll(lo, 1, 0))
        lo = jnp.where(y_low, ghost, lo)
        zu = jnp.where(z_pos < SIDE - 1, pltpu.roll(v, LANES - 1, 1), ghost)
        zl = jnp.where(z_pos > 0, pltpu.roll(v, 1, 1), ghost)
        return v, ((V[vp, j, x + 2] + V[vp, j, x]) + (up + lo)) + (zu + zl)

    def fine_rows(j, x):
        return pl.ds(x * 8 * slots + j, 8, stride=slots)

    def edges(vp, par):
        for j in range(slots):
            V[vp, j, 0] = G[par, j, 0]
            V[vp, j, SIDE + 1] = G[par, j, FOOT - 1]

    def fine_sweep(vp, par):
        @pl.loop(0, FOOT)
        def _(X):
            for j in range(slots):
                ghost = G[par, j, X]
                for e in range(2):
                    x = 2 * X + e
                    v, s = beside_fine(vp, par, j, x, ghost)
                    V[1 - vp, j, x + 1] = KEEP * v + FW[j, x] * (FS[j, x] + s)

    shrink_lane = ((lane % 32) // FOOT) * 64 + 2 * (lane % FOOT)

    def fine_remainder(vp, par, occupied):
        def body(xg, total):
            for j in range(slots):
                acc = jnp.zeros(tile, jnp.float32)
                for k in range(4):
                    X = xg * 4 + k
                    ghost = G[par, j, X]
                    t = None
                    for e in range(2):
                        x = 2 * X + e
                        v, s = beside_fine(vp, par, j, x, ghost)
                        r = (FS[j, x] - (6.0 + f_shift[fine_rows(j, x), :]) * v) + s
                        r = jnp.where(occupied[j], r, 0.0)
                        total = total + r * r
                        t = r if t is None else t + r
                    t = t + pltpu.roll(t, LANES - 1, 1)
                    t = t + pltpu.roll(t, LANES - 32, 1)
                    acc = jnp.where(lane // 32 == k, take(t, shrink_lane), acc)
                R[j, pl.ds(pl.multiple_of(xg * 8, 8), 8), :] = acc * 0.125
            return total

        return lax.fori_loop(0, FOOT // 4, body, jnp.zeros(tile, jnp.float32))

    def pack_returns():
        for q in range(group):
            which = slotid[q]
            for g in range(4):
                rows = pl.ds(g * 8, 8)
                acc = jnp.zeros(tile, jnp.float32)
                for j in range(slots):
                    acc = jnp.where(which == float(j), R[j, rows], acc)
                rout[q, rows] = acc

    def deposit():
        @pl.loop(0, FOOT // 4)
        def _(xg):
            rows = pl.ds(pl.multiple_of(xg * 8, 8), 8)
            tiles = []
            for s in range(slots):
                tiles.append(rrec[jnp.minimum(owner[0, s], group - 1), rows])
            for k in range(4):
                x = xg * 4 + k
                for yl in range(2):
                    idx = k * 32 + yl * FOOT + lane % FOOT
                    got = []
                    for s in range(slots):
                        col = jnp.where(box_live[s], box_col[s], -1)
                        got.append(jnp.where(lane // FOOT == col, take(tiles[s], idx), 0.0))
                    for b in range(along_y):
                        place = pl.ds(b * FOOT + yl, 8, stride=2)
                        acc = c_src[x, place, :]
                        for s in range(slots):
                            acc = acc + jnp.where(box_row[s] == b, got[s], 0.0)
                        comp[x, place, :] = acc

    def halo_copies(p):
        faces = (
            (U.at[p, 1], U.at[p, nx + 1]),
            (U.at[p, nx], U.at[p, 0]),
            (ys.at[0], yh.at[p, 1]),
            (ys.at[1], yh.at[p, 0]),
            (zs.at[0], zh.at[p, 1]),
            (zs.at[1], zh.at[p, 0]),
        )
        copies = []
        for i, (source, target) in enumerate(faces):
            copies.append(
                pltpu.make_async_remote_copy(
                    src_ref=source,
                    dst_ref=target,
                    send_sem=h_send.at[p, i],
                    recv_sem=h_recv.at[p, i ^ 1],
                    device_id=beside[i],
                    device_id_type=MESH,
                )
            )
        return copies

    def halo_waits(p):
        places = (
            U.at[p, 0],
            U.at[p, nx + 1],
            yh.at[p, 0],
            yh.at[p, 1],
            zh.at[p, 0],
            zh.at[p, 1],
        )
        copies = []
        for i, target in enumerate(places):
            copies.append(
                pltpu.make_async_remote_copy(
                    src_ref=target,
                    dst_ref=target,
                    send_sem=h_send.at[p, i],
                    recv_sem=h_recv.at[p, i],
                    device_id=beside[i],
                    device_id_type=MESH,
                )
            )
        return copies

    def send_halos(p):
        for i, copy in enumerate(halo_copies(p)):
            pl.when(have[i])(copy.start)

    def wait_halos(p):
        for i, (sent, got) in enumerate(zip(halo_copies(p), halo_waits(p))):

            @pl.when(have[i])
            def _():
                sent.wait_send()
                got.wait_recv()

    def keep_faces(x, u, zlo, zhi):
        ys[0, pl.ds(x, 1), :] = u[0:1]
        ys[1, pl.ds(x, 1), :] = u[ny - 1 : ny]
        zlo = jnp.where(wlane == x, u[:, 0:1], zlo)
        zhi = jnp.where(wlane == x, u[:, nz - 1 : nz], zhi)
        return zlo, zhi

    none = jnp.zeros(wide, jnp.float32)

    def coarse_sweep(p, want_faces, want_square):
        zl = zh[p, 0]
        zu = zh[p, 1]

        zlo, zhi, total = none, none, none
        for x in range(nx):
            u = U[p, x + 1]
            ym = jnp.where(wsub == 0, yh[p, 0, pl.ds(x, 1), :], pltpu.roll(u, 1, 0))
            yp = jnp.where(wsub == ny - 1, yh[p, 1, pl.ds(x, 1), :], pltpu.roll(u, ny - 1, 0))
            zm = jnp.where(wlane == 0, pltpu.roll(zl, (LANES - x) % LANES, 1) if x else zl, pltpu.roll(u, 1, 1))
            zp = jnp.where(wlane == nz - 1, pltpu.roll(zu, LANES - 1 - x, 1), pltpu.roll(u, nz - 1, 1))
            s = ((U[p, x] + U[p, x + 2]) + (ym + yp)) + (zm + zp)
            s = s + comp[x]
            new = KEEP * u + W[x] * s
            U[1 - p, x + 1] = new
            if want_square:
                last = s - (6.0 + c_shift[x]) * u
                total = total + last * last
            if want_faces:
                zlo, zhi = keep_faces(x, new, zlo, zhi)
        if want_faces:
            zs[0] = zlo
            zs[1] = zhi
        return total

    zlo, zhi = none, none
    for x in range(nx):
        u = c_start[x]
        U[0, x + 1] = u
        zlo, zhi = keep_faces(x, u, zlo, zhi)
    zs[0] = zlo
    zs[1] = zhi
    pack_parents(0)
    parent_copies = exchange(pout, prec, p_send, p_recv, 40)
    send_halos(0)

    @pl.loop(0, nx)
    def _(x):
        W[x] = OMEGA / (6.0 + c_shift[x])

    @pl.loop(0, SIDE)
    def _(x):
        for j in range(slots):
            rows = fine_rows(j, x)
            V[0, j, x + 1] = f_start[rows, :]
            FS[j, x] = f_src[rows, :]
            FW[j, x] = OMEGA / (6.0 + f_shift[rows, :])

    vp = 0
    return_copies = []
    for cycle in range(CYCLES):
        par = cycle % 2
        arrive(pout, prec, p_send, p_recv, 40)
        if cycle == 0:
            count = slot_masks()
            occupied = [count > float(j) for j in range(slots)]
        ghosts(par)
        if cycle > 0:

            @pl.loop(0, FOOT)
            def _(X):
                for j in range(slots):
                    delta = G[par, j, X] - G[1 - par, j, X]
                    for e in range(2):
                        V[vp, j, 2 * X + e + 1] = V[vp, j, 2 * X + e + 1] + delta

        edges(0, par)
        edges(1, par)
        for sweep in range(FSWEEPS):
            fine_sweep(vp, par)
            vp = 1 - vp
        square = fine_remainder(vp, par, occupied)
        for copy in return_copies:
            copy.wait_send()
        pack_returns()
        return_copies = exchange(rout, rrec, r_send, r_recv, 32)
        arrive(rout, rrec, r_send, r_recv, 32)
        deposit()
        for sweep in range(CSWEEPS):
            p = sweep % 2
            final = cycle == CYCLES - 1 and sweep == CSWEEPS - 1
            wait_halos(p)
            total = coarse_sweep(p, not final, sweep == CSWEEPS - 1)
            if not final and sweep < CSWEEPS - 1:
                send_halos(1 - p)
        for g in range(ny // 8):
            square = square + total[8 * g : 8 * g + 8]
        sums[cycle] = square
        for copy in parent_copies:
            copy.wait_send()
        pack_parents(0)
        if cycle == CYCLES - 1:
            both = jnp.where(
                sub == 0,
                jnp.sum(sums[0], axis=0, keepdims=True),
                jnp.where(sub == 1, jnp.sum(sums[1], axis=0, keepdims=True), 0.0),
            )
            for q in range(group):
                pout[q, pl.ds(32, 8)] = both
        parent_copies = exchange(pout, prec, p_send, p_recv, 40)
        if cycle < CYCLES - 1:
            send_halos(0)

    @pl.loop(0, nx)
    def _(x):
        pot_out[x] = U[0, x + 1]

    for copy in return_copies:
        copy.wait_send()
    arrive(pout, prec, p_send, p_recv, 40)
    for copy in parent_copies:
        copy.wait_send()

    mine = jnp.zeros(tile, jnp.float32)
    for q in range(group):
        mine = mine + prec[q, pl.ds(32, 8)]
    xsum[gx] = mine
    norm_copies = []
    for d in range(1, n_gx):
        copy = pltpu.make_async_remote_copy(
            src_ref=xsum.at[gx],
            dst_ref=xsum.at[gx],
            send_sem=n_send.at[d],
            recv_sem=n_recv.at[d],
            device_id=((gx + d) % n_gx, gy, gz),
            device_id_type=MESH,
        )
        copy.start()
        norm_copies.append(copy)

    par = CYCLES % 2
    ghosts(par)

    @pl.loop(0, FOOT)
    def _(X):
        for j in range(slots):
            delta = G[par, j, X] - G[1 - par, j, X]
            for e in range(2):
                x = 2 * X + e
                fine_out[fine_rows(j, x), :] = jnp.where(occupied[j], V[vp, j, x + 1] + delta, 0.0)

    for d in range(1, n_gx):
        source = (gx + n_gx - d) % n_gx
        pltpu.make_async_remote_copy(
            src_ref=xsum.at[source],
            dst_ref=xsum.at[source],
            send_sem=n_send.at[d],
            recv_sem=n_recv.at[d],
            device_id=(source, gy, gz),
            device_id_type=MESH,
        ).wait_recv()
    for copy in norm_copies:
        copy.wait_send()
    whole = jnp.zeros(tile, jnp.float32)
    for d in range(n_gx):
        whole = whole + xsum[d]
    cells = float(nx * ny * nz * n_gx * group)
    whole = jnp.sum(whole, axis=1, keepdims=True) / cells
    norm_out[...] = jnp.broadcast_to(jnp.sqrt(whole), tile)


def to_rows(a):
    slots, fine = a.shape
    return a.reshape(slots, fine // LANES, LANES).transpose(1, 0, 2).reshape(slots * fine // LANES, LANES)


def from_rows(a, slots):
    return a.reshape(-1, slots, LANES).transpose(1, 0, 2).reshape(slots, -1)


def local(sizes, c_src, c_shift, c_start, f_src, f_shift, f_start, corner, owner):
    n_gx, n_gy, n_gz = sizes
    group = n_gy * n_gz
    slots = owner.shape[1]
    nx, ny, nz = c_src.shape
    fine = f_src.shape[1]
    f32 = jnp.float32
    vmem = pl.BlockSpec(memory_space=pltpu.VMEM)
    smem = pl.BlockSpec(memory_space=pltpu.SMEM)
    dma = pltpu.SemaphoreType.DMA
    pot, rows, norms = pl.pallas_call(
        functools.partial(kernel, sizes),
        out_shape=(
            jax.ShapeDtypeStruct((nx, ny, nz), f32),
            jax.ShapeDtypeStruct((slots * fine // LANES, LANES), f32),
            jax.ShapeDtypeStruct((8, LANES), f32),
        ),
        in_specs=[smem, smem] + [vmem] * 6,
        out_specs=(vmem, vmem, vmem),
        scratch_shapes=[
            pltpu.VMEM((2, nx + 2, ny, nz), f32),
            pltpu.VMEM((nx, ny, nz), f32),
            pltpu.VMEM((nx, ny, nz), f32),
            pltpu.VMEM((2, 2, nx, nz), f32),
            pltpu.VMEM((2, nx, nz), f32),
            pltpu.VMEM((2, 2, ny, nz), f32),
            pltpu.VMEM((2, ny, nz), f32),
            pltpu.VMEM((2, slots, SIDE + 2, 8, LANES), f32),
            pltpu.VMEM((slots, SIDE, 8, LANES), f32),
            pltpu.VMEM((slots, SIDE, 8, LANES), f32),
            pltpu.VMEM((2, slots, FOOT, 8, LANES), f32),
            pltpu.VMEM((slots, 32, LANES), f32),
            pltpu.VMEM((slots, 32, LANES), f32),
            pltpu.VMEM((group, 40, LANES), f32),
            pltpu.VMEM((group, 40, LANES), f32),
            pltpu.VMEM((group, 32, LANES), f32),
            pltpu.VMEM((group, 32, LANES), f32),
            pltpu.VMEM((group, 8, LANES), f32),
            pltpu.VMEM((CYCLES, 8, LANES), f32),
            pltpu.VMEM((n_gx, 8, LANES), f32),
            dma((group,)),
            dma((group,)),
            dma((group,)),
            dma((group,)),
            dma((2, 6)),
            dma((2, 6)),
            dma((n_gx,)),
            dma((n_gx,)),
        ],
        compiler_params=pltpu.CompilerParams(collective_id=0, has_side_effects=True),
    )(corner, owner, c_src, c_shift, c_start, to_rows(f_src), to_rows(f_shift), to_rows(f_start))
    return pot, from_rows(rows, slots), norms[:CYCLES, 0]


def solution(mesh):
    sizes = (mesh.shape["gx"], mesh.shape["gy"], mesh.shape["gz"])
    everywhere = ("gx", "gy", "gz")
    block = P(*everywhere)
    in_specs = (
        block,
        block,
        block,
        P(everywhere, None),
        P(everywhere, None),
        P(everywhere, None),
        P(everywhere, None, None),
        P(everywhere, None),
    )
    out_specs = (block, P(everywhere, None), P())
    return jax.shard_map(
        functools.partial(local, sizes), mesh=mesh, in_specs=in_specs, out_specs=out_specs, check_vma=False
    )
```

```python
import functools

import jax
import jax.numpy as jnp
from jax import lax
from jax.experimental import pallas as pl
from jax.experimental.pallas import tpu as pltpu
from jax.sharding import PartitionSpec as P

FOOT = 16
CYCLES = 2
CSWEEPS = 4
FSWEEPS = 3
OMEGA = 0.8
KEEP = 1.0 - OMEGA
MESH = pl.DeviceIdType.MESH
LANES = 128
SIDE = 2 * FOOT


def take(x, idx):
    return jnp.take_along_axis(x, idx, axis=1, mode="promise_in_bounds")


def iota(shape, dim):
    return lax.broadcasted_iota(jnp.int32, shape, dim)


def kernel(
    sizes,
    corner,
    owner,
    c_src_hbm,
    c_shift_hbm,
    c_start_hbm,
    f_src_hbm,
    f_shift_hbm,
    f_start_hbm,
    pot_out,
    fine_out,
    norm_out,
    c_src,
    c_shift,
    f_src,
    f_shift,
    f_start,
    in_sem,
    U,
    W,
    comp,
    yh,
    ys,
    zh,
    zs,
    V,
    FW,
    FS,
    FD,
    G,
    compact,
    R,
    pout,
    prec,
    rout,
    rrec,
    slotid,
    sums,
    xsum,
    p_send,
    p_recv,
    r_send,
    r_recv,
    h_send,
    h_recv,
    n_send,
    n_recv,
):
    n_gx, n_gy, n_gz = sizes
    group = n_gy * n_gz
    slots = owner.shape[1]
    nx, ny, nz = c_src_hbm.shape
    along_y = ny // FOOT
    gx, gy, gz = lax.axis_index("gx"), lax.axis_index("gy"), lax.axis_index("gz")
    me = gy * n_gz + gz

    def rank_id(rank):
        return (gx, rank // n_gz, rank % n_gz)

    have = (gx > 0, gx < n_gx - 1, gy > 0, gy < n_gy - 1, gz > 0, gz < n_gz - 1)
    beside = (
        (gx - 1, gy, gz),
        (gx + 1, gy, gz),
        (gx, gy - 1, gz),
        (gx, gy + 1, gz),
        (gx, gy, gz - 1),
        (gx, gy, gz + 1),
    )

    loads = [
        pltpu.make_async_copy(source, target, in_sem.at[i])
        for i, (source, target) in enumerate(
            (
                (c_start_hbm, U.at[0, pl.ds(1, nx)]),
                (c_shift_hbm, c_shift),
                (f_start_hbm, f_start),
                (f_src_hbm, f_src),
                (f_shift_hbm, f_shift),
                (c_src_hbm, c_src),
            )
        )
    ]
    for load in loads:
        load.start()

    for p in range(2):
        U[p, 0] = jnp.zeros((ny, nz), jnp.float32)
        U[p, nx + 1] = jnp.zeros((ny, nz), jnp.float32)
    yh[...] = jnp.zeros_like(yh)
    zh[...] = jnp.zeros_like(zh)

    barrier = pltpu.get_barrier_semaphore()
    for d in range(1, group):
        pl.semaphore_signal(barrier, inc=1, device_id=rank_id((me + d) % group), device_id_type=MESH)
    for d in range(1, n_gx):
        pl.semaphore_signal(barrier, inc=1, device_id=((gx + d) % n_gx, gy, gz), device_id_type=MESH)
    pl.semaphore_wait(barrier, group - 1 + n_gx - 1)

    tile = (8, LANES)
    lane = iota(tile, 1)
    sub = iota(tile, 0)
    wide = (ny, LANES)
    wlane = iota(wide, 1)
    wsub = iota(wide, 0)
    box_row = []
    box_col = []
    box_live = []
    for s in range(slots):
        box_row.append((corner[1, 0, s] // 2 - gy * ny) // FOOT)
        box_col.append((corner[2, 0, s] // 2 - gz * nz) // FOOT)
        box_live.append(owner[0, s] < group)

    def exchange(out, rec, send, recv, rows):
        copies = []
        for d in range(1, group):
            peer = (me + d) % group
            copy = pltpu.make_async_remote_copy(
                src_ref=out.at[peer, pl.ds(0, rows)],
                dst_ref=rec.at[me, pl.ds(0, rows)],
                send_sem=send.at[d],
                recv_sem=recv.at[d],
                device_id=rank_id(peer),
                device_id_type=MESH,
            )
            copy.start()
            copies.append(copy)
        rec[me, pl.ds(0, rows)] = out[me, pl.ds(0, rows)]
        return copies

    def arrive(out, rec, send, recv, rows):
        for d in range(1, group):
            source = (me + group - d) % group
            pltpu.make_async_remote_copy(
                src_ref=out.at[source, pl.ds(0, rows)],
                dst_ref=rec.at[source, pl.ds(0, rows)],
                send_sem=send.at[d],
                recv_sem=recv.at[d],
                device_id=rank_id(source),
                device_id_type=MESH,
            ).wait_recv()

    def pack_parents(p):
        @pl.loop(0, FOOT // 4)
        def _(xg):
            for s in range(slots):
                idx = box_col[s] * FOOT + (lane % FOOT)
                acc = jnp.zeros(tile, jnp.float32)
                for k in range(4):
                    for yl in range(2):
                        a = U[p, 1 + xg * 4 + k, pl.ds(yl, 8, stride=2), :]
                        for b in range(1, along_y):
                            other = U[p, 1 + xg * 4 + k, pl.ds(b * FOOT + yl, 8, stride=2), :]
                            a = jnp.where(box_row[s] == b, other, a)
                        acc = jnp.where(lane // FOOT == 2 * k + yl, take(a, idx), acc)
                compact[s, pl.ds(pl.multiple_of(xg * 8, 8), 8), :] = acc

        for q in range(group):
            acc = jnp.zeros((32, LANES), jnp.float32)
            flag = jnp.zeros(tile, jnp.float32)
            for s in range(slots):
                acc = jnp.where(owner[0, s] == q, compact[s], acc)
                flag = jnp.where(owner[0, s] == q, 1.0, flag)
            pout[q, pl.ds(0, 32)] = acc
            pout[q, pl.ds(32, 8)] = flag

    def slot_masks():
        count = jnp.zeros(tile, jnp.float32)
        for q in range(group):
            flag = prec[q, pl.ds(32, 8)]
            slotid[q] = jnp.where(flag > 0.5, count, -1.0)
            count = count + flag
        return count

    spread_lane = (lane // 64) * FOOT + (lane % SIDE) // 2

    def ghosts(par):
        @pl.loop(0, FOOT // 4)
        def _(xg):
            rows = pl.ds(pl.multiple_of(xg * 8, 8), 8)
            for j in range(slots):
                acc = jnp.zeros(tile, jnp.float32)
                for q in range(group):
                    acc = jnp.where(slotid[q] == float(j), prec[q, rows], acc)
                for k in range(4):
                    G[par, j, xg * 4 + k] = take(acc, k * SIDE + spread_lane)

    y_top = (lane >= 96) & (sub == 7)
    y_low = (lane < 32) & (sub == 0)
    z_pos = lane % SIDE

    def plane(x, shift=0):
        start = pl.multiple_of((x + 1) * 8, 8)
        return pl.ds(start + shift, 8)

    def beside_fine(vp, par, j, x, ghost):
        v = V[vp, j, plane(x)]
        up = jnp.where(lane < 32, V[vp, j, plane(x, 1)], v)
        up = jnp.where(y_top, ghost, pltpu.roll(up, LANES - 32, 1))
        lo = jnp.where(lane >= 96, V[vp, j, plane(x, -1)], v)
        lo = jnp.where(y_low, ghost, pltpu.roll(lo, 32, 1))
        zu = jnp.where(z_pos < SIDE - 1, pltpu.roll(v, LANES - 1, 1), ghost)
        zl = jnp.where(z_pos > 0, pltpu.roll(v, 1, 1), ghost)
        return v, ((V[vp, j, plane(x + 1)] + V[vp, j, plane(x - 1)]) + (up + lo)) + (zu + zl)

    def fine_rows(j, x):
        return pl.ds(x * 8 * slots + j, 8, stride=slots)

    def edges(vp, par):
        for j in range(slots):
            V[vp, j, plane(-1)] = G[par, j, 0]
            V[vp, j, plane(SIDE)] = G[par, j, FOOT - 1]

    def fine_sweep(vp, par):
        @pl.loop(0, FOOT, unroll=4)
        def _(X):
            for j in range(slots):
                ghost = G[par, j, X]
                for e in range(2):
                    x = 2 * X + e
                    v, s = beside_fine(vp, par, j, x, ghost)
                    V[1 - vp, j, plane(x)] = KEEP * v + FW[j, x] * (FS[j, x] + s)

    shrink_lane = ((lane % 32) // FOOT) * 64 + 2 * (lane % FOOT)

    def fine_remainder(vp, par, occupied):
        def body(X, totals):
            totals = list(totals)
            for j in range(slots):
                ghost = G[par, j, X]
                for e in range(2):
                    x = 2 * X + e
                    v, s = beside_fine(vp, par, j, x, ghost)
                    r = (FS[j, x] - FD[j, x] * v) + s
                    totals[j] = totals[j] + r * r
                    V[1 - vp, j, plane(x)] = r
            return tuple(totals)

        zero = jnp.zeros(tile, jnp.float32)
        totals = lax.fori_loop(0, FOOT, body, (zero,) * slots, unroll=4)

        @pl.loop(0, FOOT // 4)
        def _(xg):
            for j in range(slots):
                acc = zero
                for k in range(4):
                    x = 2 * (xg * 4 + k)
                    t = V[1 - vp, j, plane(x)] + V[1 - vp, j, plane(x + 1)]
                    t = t + pltpu.roll(t, LANES - 1, 1)
                    t = t + pltpu.roll(t, LANES - 32, 1)
                    acc = jnp.where(lane // 32 == k, take(t, shrink_lane), acc)
                R[j, pl.ds(pl.multiple_of(xg * 8, 8), 8)] = acc * 0.125

        total = zero
        for j in range(slots):
            total = total + jnp.where(occupied[j], totals[j], 0.0)
        return total

    def pack_returns():
        for q in range(group):
            which = slotid[q]
            for g in range(4):
                rows = pl.ds(g * 8, 8)
                acc = jnp.zeros(tile, jnp.float32)
                for j in range(slots):
                    acc = jnp.where(which == float(j), R[j, rows], acc)
                rout[q, rows] = acc

    def deposit():
        @pl.loop(0, FOOT // 4)
        def _(xg):
            rows = pl.ds(pl.multiple_of(xg * 8, 8), 8)
            tiles = []
            for s in range(slots):
                tiles.append(rrec[jnp.minimum(owner[0, s], group - 1), rows])
            for k in range(4):
                x = xg * 4 + k
                for yl in range(2):
                    idx = k * 32 + yl * FOOT + lane % FOOT
                    got = []
                    for s in range(slots):
                        col = jnp.where(box_live[s], box_col[s], -1)
                        got.append(jnp.where(lane // FOOT == col, take(tiles[s], idx), 0.0))
                    for b in range(along_y):
                        place = pl.ds(b * FOOT + yl, 8, stride=2)
                        acc = c_src[x, place, :]
                        for s in range(slots):
                            acc = acc + jnp.where(box_row[s] == b, got[s], 0.0)
                        comp[x, place, :] = acc

    def halo_copies(p, which=range(6)):
        faces = (
            (U.at[p, 1], U.at[p, nx + 1]),
            (U.at[p, nx], U.at[p, 0]),
            (ys.at[0], yh.at[p, 1]),
            (ys.at[1], yh.at[p, 0]),
            (zs.at[0], zh.at[p, 1]),
            (zs.at[1], zh.at[p, 0]),
        )
        copies = []
        for i in which:
            source, target = faces[i]
            copies.append(
                pltpu.make_async_remote_copy(
                    src_ref=source,
                    dst_ref=target,
                    send_sem=h_send.at[p, i],
                    recv_sem=h_recv.at[p, i ^ 1],
                    device_id=beside[i],
                    device_id_type=MESH,
                )
            )
        return copies

    def halo_waits(p):
        places = (
            U.at[p, 0],
            U.at[p, nx + 1],
            yh.at[p, 0],
            yh.at[p, 1],
            zh.at[p, 0],
            zh.at[p, 1],
        )
        copies = []
        for i, target in enumerate(places):
            copies.append(
                pltpu.make_async_remote_copy(
                    src_ref=target,
                    dst_ref=target,
                    send_sem=h_send.at[p, i],
                    recv_sem=h_recv.at[p, i],
                    device_id=beside[i],
                    device_id_type=MESH,
                )
            )
        return copies

    def send_halos(p, which):
        for i, copy in zip(which, halo_copies(p, which)):
            pl.when(have[i])(copy.start)

    def wait_halos(p):
        for i, (sent, got) in enumerate(zip(halo_copies(p), halo_waits(p))):

            @pl.when(have[i])
            def _():
                sent.wait_send()
                got.wait_recv()

    groups = ny // 8
    per = min(groups, LANES // nx)

    def keep_y(p):
        for x in range(nx):
            ys[0, pl.ds(x, 1), :] = U[p, x + 1, pl.ds(0, 1), :]
            ys[1, pl.ds(x, 1), :] = U[p, x + 1, pl.ds(ny - 1, 1), :]

    def keep_z(p):
        for t in range(groups // per):

            def body(x, faces):
                zlo, zhi = faces
                for g in range(per):
                    at = g * nx + x
                    u = U[p, x + 1, pl.ds((t * per + g) * 8, 8)]
                    zlo = jnp.where(lane == at, pltpu.roll(u, at, 1), zlo)
                    zhi = jnp.where(lane == at, pltpu.roll(u, (at + 1) % LANES, 1), zhi)
                return zlo, zhi

            empty = jnp.zeros(tile, jnp.float32)
            zlo, zhi = lax.fori_loop(0, nx // 4, lambda i, f: body(4 * i + 3, body(4 * i + 2, body(4 * i + 1, body(4 * i, f)))), (empty, empty))
            zs[0, pl.ds(t * 8, 8)] = zlo
            zs[1, pl.ds(t * 8, 8)] = zhi

    def send_faces(p):
        send_halos(p, (0, 1))
        keep_y(p)
        send_halos(p, (2, 3))
        keep_z(p)
        send_halos(p, (4, 5))

    def z_column(packed, x, to):
        tiles = []
        for g in range(groups):
            at = (g % per) * nx + x
            face = packed[8 * (g // per) : 8 * (g // per) + 8]
            shift = (to - at) % LANES
            tiles.append(pltpu.roll(face, shift, 1) if shift else face)
        return jnp.concatenate(tiles, axis=0)

    none = jnp.zeros(wide, jnp.float32)

    def coarse_sweep(p, want_square):
        zl = zh[p, 0]
        zu = zh[p, 1]

        total = none
        for x in range(nx):
            u = U[p, x + 1]
            ym = jnp.where(wsub == 0, yh[p, 0, pl.ds(x, 1), :], pltpu.roll(u, 1, 0))
            yp = jnp.where(wsub == ny - 1, yh[p, 1, pl.ds(x, 1), :], pltpu.roll(u, ny - 1, 0))
            zm = jnp.where(wlane == 0, z_column(zl, x, 0), pltpu.roll(u, 1, 1))
            zp = jnp.where(wlane == nz - 1, z_column(zu, x, nz - 1), pltpu.roll(u, nz - 1, 1))
            s = ((U[p, x] + U[p, x + 2]) + (ym + yp)) + (zm + zp)
            s = s + comp[x]
            U[1 - p, x + 1] = KEEP * u + W[x] * s
            if want_square:
                last = s - (6.0 + c_shift[x]) * u
                total = total + last * last
        return total

    loads[0].wait()
    pack_parents(0)
    parent_copies = exchange(pout, prec, p_send, p_recv, 40)
    send_faces(0)

    for load in loads[1:]:
        load.wait()

    @pl.loop(0, nx)
    def _(x):
        W[x] = OMEGA / (6.0 + c_shift[x])

    @pl.loop(0, SIDE)
    def _(x):
        for j in range(slots):
            rows = fine_rows(j, x)
            V[0, j, plane(x)] = f_start[rows, :]
            FS[j, x] = f_src[rows, :]
            FD[j, x] = 6.0 + f_shift[rows, :]
            FW[j, x] = OMEGA / FD[j, x]

    vp = 0
    return_copies = []
    for cycle in range(CYCLES):
        par = cycle % 2
        arrive(pout, prec, p_send, p_recv, 40)
        if cycle == 0:
            count = slot_masks()
            occupied = [count > float(j) for j in range(slots)]
        ghosts(par)
        if cycle > 0:

            @pl.loop(0, FOOT)
            def _(X):
                for j in range(slots):
                    delta = G[par, j, X] - G[1 - par, j, X]
                    for e in range(2):
                        V[vp, j, plane(2 * X + e)] = V[vp, j, plane(2 * X + e)] + delta

        edges(0, par)
        edges(1, par)
        for sweep in range(FSWEEPS):
            fine_sweep(vp, par)
            vp = 1 - vp
        square = fine_remainder(vp, par, occupied)
        for copy in return_copies:
            copy.wait_send()
        pack_returns()
        return_copies = exchange(rout, rrec, r_send, r_recv, 32)
        arrive(rout, rrec, r_send, r_recv, 32)
        deposit()
        for sweep in range(CSWEEPS):
            p = sweep % 2
            final = cycle == CYCLES - 1 and sweep == CSWEEPS - 1
            wait_halos(p)
            total = coarse_sweep(p, sweep == CSWEEPS - 1)
            if not final and sweep < CSWEEPS - 1:
                send_faces(1 - p)
        for g in range(ny // 8):
            square = square + total[8 * g : 8 * g + 8]
        sums[cycle] = square
        for copy in parent_copies:
            copy.wait_send()
        pack_parents(0)
        if cycle == CYCLES - 1:
            both = jnp.where(
                sub == 0,
                jnp.sum(sums[0], axis=0, keepdims=True),
                jnp.where(sub == 1, jnp.sum(sums[1], axis=0, keepdims=True), 0.0),
            )
            for q in range(group):
                pout[q, pl.ds(32, 8)] = both
        parent_copies = exchange(pout, prec, p_send, p_recv, 40)
        if cycle < CYCLES - 1:
            send_faces(0)

    store = pltpu.make_async_copy(U.at[0, pl.ds(1, nx)], pot_out, in_sem.at[0])
    store.start()

    for copy in return_copies:
        copy.wait_send()
    arrive(pout, prec, p_send, p_recv, 40)
    for copy in parent_copies:
        copy.wait_send()

    mine = jnp.zeros(tile, jnp.float32)
    for q in range(group):
        mine = mine + prec[q, pl.ds(32, 8)]
    xsum[gx] = mine
    norm_copies = []
    for d in range(1, n_gx):
        copy = pltpu.make_async_remote_copy(
            src_ref=xsum.at[gx],
            dst_ref=xsum.at[gx],
            send_sem=n_send.at[d],
            recv_sem=n_recv.at[d],
            device_id=((gx + d) % n_gx, gy, gz),
            device_id_type=MESH,
        )
        copy.start()
        norm_copies.append(copy)

    par = CYCLES % 2
    ghosts(par)

    @pl.loop(0, FOOT)
    def _(X):
        for j in range(slots):
            delta = G[par, j, X] - G[1 - par, j, X]
            for e in range(2):
                x = 2 * X + e
                fine_out[fine_rows(j, x), :] = jnp.where(occupied[j], V[vp, j, plane(x)] + delta, 0.0)

    for d in range(1, n_gx):
        source = (gx + n_gx - d) % n_gx
        pltpu.make_async_remote_copy(
            src_ref=xsum.at[source],
            dst_ref=xsum.at[source],
            send_sem=n_send.at[d],
            recv_sem=n_recv.at[d],
            device_id=(source, gy, gz),
            device_id_type=MESH,
        ).wait_recv()
    for copy in norm_copies:
        copy.wait_send()
    store.wait()
    whole = jnp.zeros(tile, jnp.float32)
    for d in range(n_gx):
        whole = whole + xsum[d]
    cells = float(nx * ny * nz * n_gx * group)
    whole = jnp.sum(whole, axis=1, keepdims=True) / cells
    norm_out[...] = jnp.broadcast_to(jnp.sqrt(whole), tile)


def to_rows(a):
    slots, fine = a.shape
    return a.reshape(slots, fine // LANES, LANES).transpose(1, 0, 2).reshape(slots * fine // LANES, LANES)


def from_rows(a, slots):
    return a.reshape(-1, slots, LANES).transpose(1, 0, 2).reshape(slots, -1)


def local(sizes, c_src, c_shift, c_start, f_src, f_shift, f_start, corner, owner):
    n_gx, n_gy, n_gz = sizes
    group = n_gy * n_gz
    slots = owner.shape[1]
    nx, ny, nz = c_src.shape
    fine = f_src.shape[1]
    f32 = jnp.float32
    face_rows = ny // min(ny // 8, LANES // nx)
    vmem = pl.BlockSpec(memory_space=pltpu.VMEM)
    smem = pl.BlockSpec(memory_space=pltpu.SMEM)
    dma = pltpu.SemaphoreType.DMA
    pot, rows, norms = pl.pallas_call(
        functools.partial(kernel, sizes),
        out_shape=(
            jax.ShapeDtypeStruct((nx, ny, nz), f32),
            jax.ShapeDtypeStruct((slots * fine // LANES, LANES), f32),
            jax.ShapeDtypeStruct((8, LANES), f32),
        ),
        in_specs=[smem, smem] + [pl.BlockSpec(memory_space=pl.ANY)] * 6,
        out_specs=(pl.BlockSpec(memory_space=pl.ANY), vmem, vmem),
        scratch_shapes=[
            pltpu.VMEM((nx, ny, nz), f32),
            pltpu.VMEM((nx, ny, nz), f32),
            pltpu.VMEM((slots * fine // LANES, LANES), f32),
            pltpu.VMEM((slots * fine // LANES, LANES), f32),
            pltpu.VMEM((slots * fine // LANES, LANES), f32),
            dma((6,)),
            pltpu.VMEM((2, nx + 2, ny, nz), f32),
            pltpu.VMEM((nx, ny, nz), f32),
            pltpu.VMEM((nx, ny, nz), f32),
            pltpu.VMEM((2, 2, nx, nz), f32),
            pltpu.VMEM((2, nx, nz), f32),
            pltpu.VMEM((2, 2, face_rows, nz), f32),
            pltpu.VMEM((2, face_rows, nz), f32),
            pltpu.VMEM((2, slots, (SIDE + 2) * 8, LANES), f32),
            pltpu.VMEM((slots, SIDE, 8, LANES), f32),
            pltpu.VMEM((slots, SIDE, 8, LANES), f32),
            pltpu.VMEM((slots, SIDE, 8, LANES), f32),
            pltpu.VMEM((2, slots, FOOT, 8, LANES), f32),
            pltpu.VMEM((slots, 32, LANES), f32),
            pltpu.VMEM((slots, 32, LANES), f32),
            pltpu.VMEM((group, 40, LANES), f32),
            pltpu.VMEM((group, 40, LANES), f32),
            pltpu.VMEM((group, 32, LANES), f32),
            pltpu.VMEM((group, 32, LANES), f32),
            pltpu.VMEM((group, 8, LANES), f32),
            pltpu.VMEM((CYCLES, 8, LANES), f32),
            pltpu.VMEM((n_gx, 8, LANES), f32),
            dma((group,)),
            dma((group,)),
            dma((group,)),
            dma((group,)),
            dma((2, 6)),
            dma((2, 6)),
            dma((n_gx,)),
            dma((n_gx,)),
        ],
        compiler_params=pltpu.CompilerParams(collective_id=0, has_side_effects=True),
    )(corner.transpose(2, 0, 1), owner, c_src, c_shift, c_start, to_rows(f_src), to_rows(f_shift), to_rows(f_start))
    return pot, from_rows(rows, slots), norms[:CYCLES, 0]


def solution(mesh):
    sizes = (mesh.shape["gx"], mesh.shape["gy"], mesh.shape["gz"])
    everywhere = ("gx", "gy", "gz")
    block = P(*everywhere)
    in_specs = (
        block,
        block,
        block,
        P(everywhere, None),
        P(everywhere, None),
        P(everywhere, None),
        P(everywhere, None, None),
        P(everywhere, None),
    )
    out_specs = (block, P(everywhere, None), P())
    return jax.shard_map(
        functools.partial(local, sizes), mesh=mesh, in_specs=in_specs, out_specs=out_specs, check_vma=False
    )
```

```python
import functools

import jax
import jax.numpy as jnp
from jax import lax
from jax.experimental import pallas as pl
from jax.experimental.pallas import tpu as pltpu
from jax.sharding import PartitionSpec as P

FOOT = 16
CYCLES = 2
CSWEEPS = 4
FSWEEPS = 3
OMEGA = 0.8
KEEP = 1.0 - OMEGA
MESH = pl.DeviceIdType.MESH
LANES = 128
SIDE = 2 * FOOT


def take(x, idx):
    return jnp.take_along_axis(x, idx, axis=1, mode="promise_in_bounds")


def iota(shape, dim):
    return lax.broadcasted_iota(jnp.int32, shape, dim)


def kernel(
    sizes,
    corner,
    owner,
    c_src_hbm,
    c_shift_hbm,
    c_start_hbm,
    f_src_hbm,
    f_shift_hbm,
    f_start_hbm,
    pot_out,
    fine_out,
    norm_out,
    c_src,
    c_shift,
    f_src,
    f_shift,
    f_start,
    in_sem,
    U,
    W,
    comp,
    yh,
    ys,
    zh,
    zs,
    V,
    FW,
    FS,
    FD,
    G,
    compact,
    R,
    pout,
    prec,
    rout,
    rrec,
    slotid,
    sums,
    xsum,
    p_send,
    p_recv,
    r_send,
    r_recv,
    h_send,
    h_recv,
    n_send,
    n_recv,
):
    n_gx, n_gy, n_gz = sizes
    group = n_gy * n_gz
    slots = owner.shape[1]
    nx, ny, nz = c_src_hbm.shape
    along_y = ny // FOOT
    gx, gy, gz = lax.axis_index("gx"), lax.axis_index("gy"), lax.axis_index("gz")
    me = gy * n_gz + gz

    def rank_id(rank):
        return (gx, rank // n_gz, rank % n_gz)

    have = (gx > 0, gx < n_gx - 1, gy > 0, gy < n_gy - 1, gz > 0, gz < n_gz - 1)
    beside = (
        (gx - 1, gy, gz),
        (gx + 1, gy, gz),
        (gx, gy - 1, gz),
        (gx, gy + 1, gz),
        (gx, gy, gz - 1),
        (gx, gy, gz + 1),
    )

    loads = [
        pltpu.make_async_copy(source, target, in_sem.at[i])
        for i, (source, target) in enumerate(
            (
                (c_start_hbm, U.at[0, pl.ds(1, nx)]),
                (c_shift_hbm, c_shift),
                (f_start_hbm, f_start),
                (f_src_hbm, f_src),
                (f_shift_hbm, f_shift),
                (c_src_hbm, c_src),
            )
        )
    ]
    for load in loads:
        load.start()

    for p in range(2):
        U[p, 0] = jnp.zeros((ny, nz), jnp.float32)
        U[p, nx + 1] = jnp.zeros((ny, nz), jnp.float32)
    yh[...] = jnp.zeros_like(yh)
    zh[...] = jnp.zeros_like(zh)

    barrier = pltpu.get_barrier_semaphore()
    for d in range(1, group):
        pl.semaphore_signal(barrier, inc=1, device_id=rank_id((me + d) % group), device_id_type=MESH)
    for d in range(1, n_gx):
        pl.semaphore_signal(barrier, inc=1, device_id=((gx + d) % n_gx, gy, gz), device_id_type=MESH)
    pl.semaphore_wait(barrier, group - 1 + n_gx - 1)

    tile = (8, LANES)
    lane = iota(tile, 1)
    sub = iota(tile, 0)
    wide = (ny, LANES)
    wlane = iota(wide, 1)
    wsub = iota(wide, 0)
    box_row = []
    box_col = []
    box_live = []
    for s in range(slots):
        box_row.append((corner[1, 0, s] // 2 - gy * ny) // FOOT)
        box_col.append((corner[2, 0, s] // 2 - gz * nz) // FOOT)
        box_live.append(owner[0, s] < group)

    def exchange(out, rec, send, recv, rows):
        copies = []
        for d in range(1, group):
            peer = (me + d) % group
            copy = pltpu.make_async_remote_copy(
                src_ref=out.at[peer, pl.ds(0, rows)],
                dst_ref=rec.at[me, pl.ds(0, rows)],
                send_sem=send.at[d],
                recv_sem=recv.at[d],
                device_id=rank_id(peer),
                device_id_type=MESH,
            )
            copy.start()
            copies.append(copy)
        rec[me, pl.ds(0, rows)] = out[me, pl.ds(0, rows)]
        return copies

    def arrive(out, rec, send, recv, rows):
        for d in range(1, group):
            source = (me + group - d) % group
            pltpu.make_async_remote_copy(
                src_ref=out.at[source, pl.ds(0, rows)],
                dst_ref=rec.at[source, pl.ds(0, rows)],
                send_sem=send.at[d],
                recv_sem=recv.at[d],
                device_id=rank_id(source),
                device_id_type=MESH,
            ).wait_recv()

    def pack_parents(p):
        @pl.loop(0, FOOT // 4)
        def _(xg):
            for s in range(slots):
                idx = box_col[s] * FOOT + (lane % FOOT)
                acc = jnp.zeros(tile, jnp.float32)
                for k in range(4):
                    for yl in range(2):
                        a = U[p, 1 + xg * 4 + k, pl.ds(yl, 8, stride=2), :]
                        for b in range(1, along_y):
                            other = U[p, 1 + xg * 4 + k, pl.ds(b * FOOT + yl, 8, stride=2), :]
                            a = jnp.where(box_row[s] == b, other, a)
                        acc = jnp.where(lane // FOOT == 2 * k + yl, take(a, idx), acc)
                compact[s, pl.ds(pl.multiple_of(xg * 8, 8), 8), :] = acc

        for q in range(group):
            acc = jnp.zeros((32, LANES), jnp.float32)
            flag = jnp.zeros(tile, jnp.float32)
            for s in range(slots):
                acc = jnp.where(owner[0, s] == q, compact[s], acc)
                flag = jnp.where(owner[0, s] == q, 1.0, flag)
            pout[q, pl.ds(0, 32)] = acc
            pout[q, pl.ds(32, 8)] = flag

    def slot_masks():
        count = jnp.zeros(tile, jnp.float32)
        for q in range(group):
            flag = prec[q, pl.ds(32, 8)]
            slotid[q] = jnp.where(flag > 0.5, count, -1.0)
            count = count + flag
        return count

    spread_lane = (lane // 64) * FOOT + (lane % SIDE) // 2

    def ghosts(par):
        @pl.loop(0, FOOT // 4)
        def _(xg):
            rows = pl.ds(pl.multiple_of(xg * 8, 8), 8)
            for j in range(slots):
                acc = jnp.zeros(tile, jnp.float32)
                for q in range(group):
                    acc = jnp.where(slotid[q] == float(j), prec[q, rows], acc)
                for k in range(4):
                    G[par, j, xg * 4 + k] = take(acc, k * SIDE + spread_lane)

    y_top = (lane >= 96) & (sub == 7)
    y_low = (lane < 32) & (sub == 0)
    z_pos = lane % SIDE

    def plane(x, shift=0):
        start = pl.multiple_of((x + 1) * 8, 8)
        return pl.ds(start + shift, 8)

    def beside_fine(vp, par, j, x, ghost):
        v = V[vp, j, plane(x)]
        up = jnp.where(lane < 32, V[vp, j, plane(x, 1)], v)
        up = jnp.where(y_top, ghost, pltpu.roll(up, LANES - 32, 1))
        lo = jnp.where(lane >= 96, V[vp, j, plane(x, -1)], v)
        lo = jnp.where(y_low, ghost, pltpu.roll(lo, 32, 1))
        zu = jnp.where(z_pos < SIDE - 1, pltpu.roll(v, LANES - 1, 1), ghost)
        zl = jnp.where(z_pos > 0, pltpu.roll(v, 1, 1), ghost)
        return v, ((V[vp, j, plane(x + 1)] + V[vp, j, plane(x - 1)]) + (up + lo)) + (zu + zl)

    def fine_rows(j, x):
        return pl.ds(x * 8 * slots + j, 8, stride=slots)

    def edges(vp, par):
        for j in range(slots):
            V[vp, j, plane(-1)] = G[par, j, 0]
            V[vp, j, plane(SIDE)] = G[par, j, FOOT - 1]

    def fine_sweep(vp, par):
        @pl.loop(0, FOOT, unroll=4)
        def _(X):
            for j in range(slots):
                ghost = G[par, j, X]
                for e in range(2):
                    x = 2 * X + e
                    v, s = beside_fine(vp, par, j, x, ghost)
                    V[1 - vp, j, plane(x)] = KEEP * v + FW[j, x] * (FS[j, x] + s)

    shrink_lane = ((lane % 32) // FOOT) * 64 + 2 * (lane % FOOT)

    def fine_remainder(vp, par, occupied):
        def body(X, totals):
            totals = list(totals)
            for j in range(slots):
                ghost = G[par, j, X]
                for e in range(2):
                    x = 2 * X + e
                    v, s = beside_fine(vp, par, j, x, ghost)
                    r = (FS[j, x] - FD[j, x] * v) + s
                    totals[j] = totals[j] + r * r
                    V[1 - vp, j, plane(x)] = r
            return tuple(totals)

        zero = jnp.zeros(tile, jnp.float32)
        totals = lax.fori_loop(0, FOOT, body, (zero,) * slots, unroll=4)

        @pl.loop(0, FOOT // 4)
        def _(xg):
            for j in range(slots):
                acc = zero
                for k in range(4):
                    x = 2 * (xg * 4 + k)
                    t = V[1 - vp, j, plane(x)] + V[1 - vp, j, plane(x + 1)]
                    t = t + pltpu.roll(t, LANES - 1, 1)
                    t = t + pltpu.roll(t, LANES - 32, 1)
                    acc = jnp.where(lane // 32 == k, take(t, shrink_lane), acc)
                R[j, pl.ds(pl.multiple_of(xg * 8, 8), 8)] = acc * 0.125

        total = zero
        for j in range(slots):
            total = total + jnp.where(occupied[j], totals[j], 0.0)
        return total

    def pack_returns():
        for q in range(group):
            which = slotid[q]
            for g in range(4):
                rows = pl.ds(g * 8, 8)
                acc = jnp.zeros(tile, jnp.float32)
                for j in range(slots):
                    acc = jnp.where(which == float(j), R[j, rows], acc)
                rout[q, rows] = acc

    def deposit():
        @pl.loop(0, FOOT // 4)
        def _(xg):
            rows = pl.ds(pl.multiple_of(xg * 8, 8), 8)
            tiles = []
            for s in range(slots):
                tiles.append(rrec[jnp.minimum(owner[0, s], group - 1), rows])
            for k in range(4):
                x = xg * 4 + k
                for yl in range(2):
                    idx = k * 32 + yl * FOOT + lane % FOOT
                    got = []
                    for s in range(slots):
                        col = jnp.where(box_live[s], box_col[s], -1)
                        got.append(jnp.where(lane // FOOT == col, take(tiles[s], idx), 0.0))
                    for b in range(along_y):
                        place = pl.ds(b * FOOT + yl, 8, stride=2)
                        acc = c_src[x, place, :]
                        for s in range(slots):
                            acc = acc + jnp.where(box_row[s] == b, got[s], 0.0)
                        comp[x, place, :] = acc

    def halo_copies(p, which=range(6)):
        faces = (
            (U.at[p, 1], U.at[p, nx + 1]),
            (U.at[p, nx], U.at[p, 0]),
            (ys.at[0], yh.at[p, 1]),
            (ys.at[1], yh.at[p, 0]),
            (zs.at[0], zh.at[p, 1]),
            (zs.at[1], zh.at[p, 0]),
        )
        copies = []
        for i in which:
            source, target = faces[i]
            copies.append(
                pltpu.make_async_remote_copy(
                    src_ref=source,
                    dst_ref=target,
                    send_sem=h_send.at[p, i],
                    recv_sem=h_recv.at[p, i ^ 1],
                    device_id=beside[i],
                    device_id_type=MESH,
                )
            )
        return copies

    def halo_waits(p):
        places = (
            U.at[p, 0],
            U.at[p, nx + 1],
            yh.at[p, 0],
            yh.at[p, 1],
            zh.at[p, 0],
            zh.at[p, 1],
        )
        copies = []
        for i, target in enumerate(places):
            copies.append(
                pltpu.make_async_remote_copy(
                    src_ref=target,
                    dst_ref=target,
                    send_sem=h_send.at[p, i],
                    recv_sem=h_recv.at[p, i],
                    device_id=beside[i],
                    device_id_type=MESH,
                )
            )
        return copies

    def send_halos(p, which):
        for i, copy in zip(which, halo_copies(p, which)):
            pl.when(have[i])(copy.start)

    def wait_halos(p):
        for i, (sent, got) in enumerate(zip(halo_copies(p), halo_waits(p))):

            @pl.when(have[i])
            def _():
                sent.wait_send()
                got.wait_recv()

    groups = ny // 8
    per = min(groups, LANES // nx)

    def keep_y(p):
        for x in range(nx):
            ys[0, pl.ds(x, 1), :] = U[p, x + 1, pl.ds(0, 1), :]
            ys[1, pl.ds(x, 1), :] = U[p, x + 1, pl.ds(ny - 1, 1), :]

    def keep_z(p):
        for t in range(groups // per):

            def body(x, faces):
                zlo, zhi = faces
                for g in range(per):
                    at = g * nx + x
                    u = U[p, x + 1, pl.ds((t * per + g) * 8, 8)]
                    zlo = jnp.where(lane == at, pltpu.roll(u, at, 1), zlo)
                    zhi = jnp.where(lane == at, pltpu.roll(u, (at + 1) % LANES, 1), zhi)
                return zlo, zhi

            empty = jnp.zeros(tile, jnp.float32)
            zlo, zhi = lax.fori_loop(0, nx // 4, lambda i, f: body(4 * i + 3, body(4 * i + 2, body(4 * i + 1, body(4 * i, f)))), (empty, empty))
            zs[0, pl.ds(t * 8, 8)] = zlo
            zs[1, pl.ds(t * 8, 8)] = zhi

    def send_faces(p):
        send_halos(p, (0, 1))
        keep_y(p)
        send_halos(p, (2, 3))
        keep_z(p)
        send_halos(p, (4, 5))

    def z_column(packed, x, to):
        tiles = []
        for g in range(groups):
            at = (g % per) * nx + x
            face = packed[8 * (g // per) : 8 * (g // per) + 8]
            shift = (to - at) % LANES
            tiles.append(pltpu.roll(face, shift, 1) if shift else face)
        return jnp.concatenate(tiles, axis=0)

    none = jnp.zeros(wide, jnp.float32)

    def coarse_sweep(p, want_square):
        zl = zh[p, 0]
        zu = zh[p, 1]

        total = none
        for x in range(nx):
            u = U[p, x + 1]
            ym = jnp.where(wsub == 0, yh[p, 0, pl.ds(x, 1), :], pltpu.roll(u, 1, 0))
            yp = jnp.where(wsub == ny - 1, yh[p, 1, pl.ds(x, 1), :], pltpu.roll(u, ny - 1, 0))
            zm = jnp.where(wlane == 0, z_column(zl, x, 0), pltpu.roll(u, 1, 1))
            zp = jnp.where(wlane == nz - 1, z_column(zu, x, nz - 1), pltpu.roll(u, nz - 1, 1))
            s = ((U[p, x] + U[p, x + 2]) + (ym + yp)) + (zm + zp)
            s = s + comp[x]
            U[1 - p, x + 1] = KEEP * u + W[x] * s
            if want_square:
                last = s - (6.0 + c_shift[x]) * u
                total = total + last * last
        return total

    loads[0].wait()
    pack_parents(0)
    parent_copies = exchange(pout, prec, p_send, p_recv, 40)
    send_faces(0)

    for load in loads[1:]:
        load.wait()

    @pl.loop(0, nx)
    def _(x):
        W[x] = OMEGA / (6.0 + c_shift[x])

    @pl.loop(0, SIDE)
    def _(x):
        for j in range(slots):
            rows = fine_rows(j, x)
            V[0, j, plane(x)] = f_start[rows, :]
            FS[j, x] = f_src[rows, :]
            FD[j, x] = 6.0 + f_shift[rows, :]
            FW[j, x] = OMEGA / FD[j, x]

    vp = 0
    return_copies = []
    for cycle in range(CYCLES):
        par = cycle % 2
        arrive(pout, prec, p_send, p_recv, 40)
        if cycle == 0:
            count = slot_masks()
            occupied = [count > float(j) for j in range(slots)]
        ghosts(par)
        if cycle > 0:

            @pl.loop(0, FOOT)
            def _(X):
                for j in range(slots):
                    delta = G[par, j, X] - G[1 - par, j, X]
                    for e in range(2):
                        V[vp, j, plane(2 * X + e)] = V[vp, j, plane(2 * X + e)] + delta

        edges(0, par)
        edges(1, par)
        for sweep in range(FSWEEPS):
            fine_sweep(vp, par)
            vp = 1 - vp
        square = fine_remainder(vp, par, occupied)
        for copy in return_copies:
            copy.wait_send()
        pack_returns()
        return_copies = exchange(rout, rrec, r_send, r_recv, 32)
        arrive(rout, rrec, r_send, r_recv, 32)
        deposit()
        for sweep in range(CSWEEPS):
            p = sweep % 2
            final = cycle == CYCLES - 1 and sweep == CSWEEPS - 1
            wait_halos(p)
            total = coarse_sweep(p, sweep == CSWEEPS - 1)
            if not final and sweep < CSWEEPS - 1:
                send_faces(1 - p)
        for g in range(ny // 8):
            square = square + total[8 * g : 8 * g + 8]
        sums[cycle] = square
        for copy in parent_copies:
            copy.wait_send()
        pack_parents(0)
        if cycle == CYCLES - 1:
            both = jnp.where(
                sub == 0,
                jnp.sum(sums[0], axis=0, keepdims=True),
                jnp.where(sub == 1, jnp.sum(sums[1], axis=0, keepdims=True), 0.0),
            )
            for q in range(group):
                pout[q, pl.ds(32, 8)] = both
        parent_copies = exchange(pout, prec, p_send, p_recv, 40)
        if cycle < CYCLES - 1:
            send_faces(0)

    store = pltpu.make_async_copy(U.at[0, pl.ds(1, nx)], pot_out, in_sem.at[0])
    store.start()

    for copy in return_copies:
        copy.wait_send()
    arrive(pout, prec, p_send, p_recv, 40)
    for copy in parent_copies:
        copy.wait_send()

    mine = jnp.zeros(tile, jnp.float32)
    for q in range(group):
        mine = mine + prec[q, pl.ds(32, 8)]
    xsum[gx] = mine
    norm_copies = []
    for d in range(1, n_gx):
        copy = pltpu.make_async_remote_copy(
            src_ref=xsum.at[gx],
            dst_ref=xsum.at[gx],
            send_sem=n_send.at[d],
            recv_sem=n_recv.at[d],
            device_id=((gx + d) % n_gx, gy, gz),
            device_id_type=MESH,
        )
        copy.start()
        norm_copies.append(copy)

    par = CYCLES % 2
    ghosts(par)

    @pl.loop(0, FOOT)
    def _(X):
        for j in range(slots):
            delta = G[par, j, X] - G[1 - par, j, X]
            for e in range(2):
                x = 2 * X + e
                fine_out[fine_rows(j, x), :] = jnp.where(occupied[j], V[vp, j, plane(x)] + delta, 0.0)

    for d in range(1, n_gx):
        source = (gx + n_gx - d) % n_gx
        pltpu.make_async_remote_copy(
            src_ref=xsum.at[source],
            dst_ref=xsum.at[source],
            send_sem=n_send.at[d],
            recv_sem=n_recv.at[d],
            device_id=(source, gy, gz),
            device_id_type=MESH,
        ).wait_recv()
    for copy in norm_copies:
        copy.wait_send()
    store.wait()
    whole = jnp.zeros(tile, jnp.float32)
    for d in range(n_gx):
        whole = whole + xsum[d]
    cells = float(nx * ny * nz * n_gx * group)
    whole = jnp.sum(whole, axis=1, keepdims=True) / cells
    norm_out[...] = jnp.broadcast_to(jnp.sqrt(whole), tile)


def finish(pieces, norms, pot, rows, pot_out, rows_out, norm_out, pot_buf, rows_buf, in_sem, out_sem):
    parts = []
    for k, (source, buf, target) in enumerate(((rows, rows_buf, rows_out), (pot, pot_buf, pot_out))):
        count = source.shape[0] // pieces
        for i in range(pieces):
            at = pl.ds(i * count, count)
            n = k * pieces + i
            parts.append(
                (
                    pltpu.make_async_copy(source.at[at], buf.at[at], in_sem.at[n]),
                    pltpu.make_async_copy(buf.at[at], target.at[at], out_sem.at[n]),
                )
            )
    for load, _ in parts:
        load.start()
    for k in range(CYCLES):
        norm_out[k] = norms[k, 0]
    for load, store in parts:
        load.wait()
        store.start()
    for _, store in parts:
        store.wait()


def to_rows(a):
    slots, fine = a.shape
    return a.reshape(slots, fine // LANES, LANES).transpose(1, 0, 2).reshape(slots * fine // LANES, LANES)


def from_rows(a, slots):
    return a.reshape(-1, slots, LANES).transpose(1, 0, 2).reshape(slots, -1)


def local(sizes, c_src, c_shift, c_start, f_src, f_shift, f_start, corner, owner):
    n_gx, n_gy, n_gz = sizes
    group = n_gy * n_gz
    slots = owner.shape[1]
    nx, ny, nz = c_src.shape
    fine = f_src.shape[1]
    f32 = jnp.float32
    face_rows = ny // min(ny // 8, LANES // nx)
    vmem = pl.BlockSpec(memory_space=pltpu.VMEM)
    smem = pl.BlockSpec(memory_space=pltpu.SMEM)
    dma = pltpu.SemaphoreType.DMA
    pot, rows, norms = pl.pallas_call(
        functools.partial(kernel, sizes),
        out_shape=(
            jax.ShapeDtypeStruct((nx, ny, nz), f32),
            jax.ShapeDtypeStruct((slots * fine // LANES, LANES), f32),
            jax.ShapeDtypeStruct((8, LANES), f32),
        ),
        in_specs=[smem, smem] + [pl.BlockSpec(memory_space=pl.ANY)] * 6,
        out_specs=(pl.BlockSpec(memory_space=pl.ANY), vmem, vmem),
        scratch_shapes=[
            pltpu.VMEM((nx, ny, nz), f32),
            pltpu.VMEM((nx, ny, nz), f32),
            pltpu.VMEM((slots * fine // LANES, LANES), f32),
            pltpu.VMEM((slots * fine // LANES, LANES), f32),
            pltpu.VMEM((slots * fine // LANES, LANES), f32),
            dma((6,)),
            pltpu.VMEM((2, nx + 2, ny, nz), f32),
            pltpu.VMEM((nx, ny, nz), f32),
            pltpu.VMEM((nx, ny, nz), f32),
            pltpu.VMEM((2, 2, nx, nz), f32),
            pltpu.VMEM((2, nx, nz), f32),
            pltpu.VMEM((2, 2, face_rows, nz), f32),
            pltpu.VMEM((2, face_rows, nz), f32),
            pltpu.VMEM((2, slots, (SIDE + 2) * 8, LANES), f32),
            pltpu.VMEM((slots, SIDE, 8, LANES), f32),
            pltpu.VMEM((slots, SIDE, 8, LANES), f32),
            pltpu.VMEM((slots, SIDE, 8, LANES), f32),
            pltpu.VMEM((2, slots, FOOT, 8, LANES), f32),
            pltpu.VMEM((slots, 32, LANES), f32),
            pltpu.VMEM((slots, 32, LANES), f32),
            pltpu.VMEM((group, 40, LANES), f32),
            pltpu.VMEM((group, 40, LANES), f32),
            pltpu.VMEM((group, 32, LANES), f32),
            pltpu.VMEM((group, 32, LANES), f32),
            pltpu.VMEM((group, 8, LANES), f32),
            pltpu.VMEM((CYCLES, 8, LANES), f32),
            pltpu.VMEM((n_gx, 8, LANES), f32),
            dma((group,)),
            dma((group,)),
            dma((group,)),
            dma((group,)),
            dma((2, 6)),
            dma((2, 6)),
            dma((n_gx,)),
            dma((n_gx,)),
        ],
        compiler_params=pltpu.CompilerParams(collective_id=0, has_side_effects=True),
    )(corner.transpose(2, 0, 1), owner, c_src, c_shift, c_start, to_rows(f_src), to_rows(f_shift), to_rows(f_start))
    pieces = 2
    anywhere = pl.BlockSpec(memory_space=pl.ANY)
    pot, rows, norms = pl.pallas_call(
        functools.partial(finish, pieces),
        out_shape=(
            jax.ShapeDtypeStruct(pot.shape, f32),
            jax.ShapeDtypeStruct(rows.shape, f32),
            jax.ShapeDtypeStruct((CYCLES,), f32),
        ),
        in_specs=[smem, anywhere, anywhere],
        out_specs=(anywhere, anywhere, smem),
        scratch_shapes=[
            pltpu.VMEM(pot.shape, f32),
            pltpu.VMEM(rows.shape, f32),
            dma((2 * pieces,)),
            dma((2 * pieces,)),
        ],
    )(norms, pot, rows)
    return pot, from_rows(rows, slots), norms


def solution(mesh):
    sizes = (mesh.shape["gx"], mesh.shape["gy"], mesh.shape["gz"])
    everywhere = ("gx", "gy", "gz")
    block = P(*everywhere)
    in_specs = (
        block,
        block,
        block,
        P(everywhere, None),
        P(everywhere, None),
        P(everywhere, None),
        P(everywhere, None, None),
        P(everywhere, None),
    )
    out_specs = (block, P(everywhere, None), P())
    return jax.shard_map(
        functools.partial(local, sizes), mesh=mesh, in_specs=in_specs, out_specs=out_specs, check_vma=False
    )
```
